512 devices in a mesh: gx: 32 (over z, core), gy: 16 (over y, x).
Axes of the slice: x: 4, y: 4, z: 16, core: 2. Of those that a mesh axis runs over, the one named last changes fastest.
Arguments:
- bin_state: float32 [132, 256, 2048], P(None, 'gx', 'gy'), may hold values from 0.05 to 2
- courant_x: float32 [256, 2048], P('gx', 'gy'), may hold values from -0.4 to 0.4
- courant_y: float32 [256, 2048], P('gx', 'gy'), may hold values from -0.4 to 0.4
- cloudy_order: int32 [32, 16, 8], P('gx', 'gy'), may hold values from 0 to 7, each once within a row
- block_count: int32 [16, 32], P('gy', 'gx'), may hold values from 1 to 8, 160 in all within a row
- gain_kernel: bfloat16 [10, 33, 1089], replicated, may hold values from -0.059814453 to 0.059814453
- loss_rate: bfloat16 [10, 33, 33], replicated, may hold values from 9.9658966e-05 to 0.029907227
Outputs:
- state_out: float32 [132, 256, 2048], P(None, 'gx', 'gy')
The draws below stay inside these ranges and needn't reach their ends.
Inputs may be any that keep to these rules, and one draw needn't show every extreme that they name: `cloudy_order`: each device's row holds each of its 8 block numbers once. `block_count`: each row of 32 counts sums to 160, and its largest count is 8.
All inputs are finite; a program needn't handle non-finite values. No bound on the sum of `block_count` on one device may be relied on, other than what follows from the above.
Results may differ from the reference program's by a relative error of at most 0.0034.
Values may be sent and summed in bfloat16 or wider, within the bound.
A program may use at most 128 MiB of HBM per device.

```python
import math
import jax
import jax.numpy as jnp
import numpy as np
from jax import lax

BINS = 33
CLASSES = 4
PAIRS = 10
COMPS = 132
LEV = 4
BLOCK = 128
CX = 8
STEPS = 2
MEANB = 5
MAXB = 8
NX = 256
NY = 512
N_GX = 32
N_GY = 16


def block_levels(stream_key, extent, split, smallest, high):
    factor_of, own = 1.0, jax.random.fold_in(stream_key, 6)
    for position, parts in split:
        heights = jnp.exp(jax.random.uniform(jax.random.fold_in(own, position), (parts,), jnp.float32, smallest / len(split), high / len(split)))
        factor_of = factor_of * jnp.repeat(heights, extent[position] // parts).reshape([-1 if axis == position else 1 for axis in range(len(extent))])
    return factor_of


def profile(count, total, bound, lean):
    portions = [(1 << 20) // math.isqrt(rank ** lean) + 1 for rank in range(2, count + 1)]
    rest, given = total - bound - (count - 1), [1] * (count - 1)
    while rest > 0:
        movable = [i for i in range(count - 1) if given[i] < bound]
        pool, remaining = sum([portions[i] for i in movable]), rest
        for i in movable:
            extra = min(bound - given[i], max(1, remaining * portions[i] // pool), rest)
            given[i] = given[i] + extra
            rest = rest - extra
    return np.array([bound] + given)


def uneven_parts(own_key, number_of, total, reach, skew):
    if number_of == 2:
        one = jax.random.randint(own_key, (), max(1, total - reach), min(reach, total - 1) + 1)
        return jnp.stack([one, total - one])
    tallies = jnp.asarray(profile(number_of, total, reach, skew), jnp.int32)
    couples = (number_of - 1) // 2
    donor, receiver = tallies[1:1 + 2 * couples:2], tallies[2:2 + 2 * couples:2]
    margin = jnp.minimum(donor - 1, reach - receiver)
    passed = jax.random.randint(jax.random.fold_in(own_key, 1), (couples,), 0, 1 << 20) % (margin + 1)
    tallies = tallies.at[1:1 + 2 * couples:2].set(donor - passed).at[2:2 + 2 * couples:2].set(receiver + passed)
    return tallies[jax.random.permutation(jax.random.fold_in(own_key, 2), number_of)]


def bell_draw(rng, extent, width, reach, kind=jnp.bfloat16):
    return jnp.clip(width * jax.random.normal(rng, extent, jnp.float32), -reach, reach).astype(kind)


def setup_inputs(seed: int = 0) -> dict:
    arg_keys = jax.random.split(jax.random.key(seed), 8)
    bin_state = jnp.clip(jnp.exp(math.log(2.0) - 3.6888794 * jax.random.uniform(arg_keys[0], (COMPS, NX, NY * LEV), jnp.float32) ** block_levels(arg_keys[0], (COMPS, NX, NY * LEV), ((1, 32), (2, 16)), -0.2, 0.2)), 0.05, 2.0)
    courant_x = jnp.clip(jax.random.uniform(arg_keys[1], (NX, NY * LEV), jnp.float32, -0.4, 0.4) * block_levels(arg_keys[1], (NX, NY * LEV), ((0, 32), (1, 16)), -0.4, 0.0), -0.4, 0.4)
    courant_y = jnp.clip(jax.random.uniform(arg_keys[2], (NX, NY * LEV), jnp.float32, -0.4, 0.4) * block_levels(arg_keys[2], (NX, NY * LEV), ((0, 32), (1, 16)), -0.4, 0.0), -0.4, 0.4)
    cloudy_order = jax.vmap(lambda own: jax.random.permutation(own, CX))(jax.random.split(arg_keys[3], N_GX * N_GY)).reshape((N_GX, N_GY, CX)).astype(jnp.int32)
    block_count = jax.vmap(lambda own: uneven_parts(own, N_GX, N_GX * MEANB, MAXB, 2))(jax.random.split(arg_keys[4], N_GY)).reshape((N_GY, N_GX)).astype(jnp.int32)
    gain_kernel = bell_draw(arg_keys[5], (PAIRS, BINS, BINS * BINS), 0.01, 0.059814453)
    loss_rate = jnp.clip(jnp.exp(jax.random.uniform(arg_keys[6], (PAIRS, BINS, BINS), jnp.float32, math.log(9.965896606445312e-05), math.log(0.029907227))), 9.965896606445312e-05, 0.029907227).astype(jnp.bfloat16)
    return {"bin_state": bin_state, "courant_x": courant_x, "courant_y": courant_y, "cloudy_order": cloudy_order, "block_count": block_count, "gain_kernel": gain_kernel, "loss_rate": loss_rate}


pair_table = ((0, 0, 1), (0, 1, 1), (0, 2, 2), (0, 3, 3), (1, 1, 1), (1, 2, 3), (1, 3, 3), (2, 2, 3), (2, 3, 3), (3, 3, 3))


def upwind(centre, minus_one, minus_two, plus_one, plus_two, courant):
    rising = (2.0 * plus_one + 3.0 * centre - 6.0 * minus_one + minus_two) / 6.0
    falling = (6.0 * plus_one - plus_two - 3.0 * centre - 2.0 * minus_one) / 6.0
    return jnp.where(courant > 0.0, rising, falling)


def transport(component, courant_x, courant_y):
    along_x = upwind(component, jnp.roll(component, 1, 0), jnp.roll(component, 2, 0), jnp.roll(component, -1, 0), jnp.roll(component, -2, 0), courant_x)
    along_y = upwind(component, jnp.roll(component, LEV, 1), jnp.roll(component, 2 * LEV, 1), jnp.roll(component, -LEV, 1), jnp.roll(component, -2 * LEV, 1), courant_y)
    return jnp.maximum(component - courant_x * along_x - courant_y * along_y, 0.0)


def collide(bin_values, gain_kernel, loss_rate):
    column_count = bin_values.shape[1]
    tendency = [jnp.zeros((BINS, column_count), jnp.float32) for member in range(CLASSES)]
    for pair_index, (former, latter, target) in enumerate(pair_table):
        former_bins = bin_values[former * BINS:(former + 1) * BINS].astype(jnp.float32)
        latter_bins = bin_values[latter * BINS:(latter + 1) * BINS].astype(jnp.float32)
        product = (former_bins[:, None, :] * latter_bins[None, :, :]).reshape(BINS * BINS, column_count)
        product = product.astype(jnp.bfloat16).astype(jnp.float32)
        kernel = gain_kernel[pair_index].astype(jnp.float32)
        rates = loss_rate[pair_index].astype(jnp.float32)
        tendency[target] = tendency[target] + jnp.dot(kernel, product, precision=lax.Precision.HIGHEST, preferred_element_type=jnp.float32)
        tendency[former] = tendency[former] - former_bins * jnp.dot(rates, latter_bins, precision=lax.Precision.HIGHEST, preferred_element_type=jnp.float32)
        tendency[latter] = tendency[latter] - latter_bins * jnp.dot(rates.T, former_bins, precision=lax.Precision.HIGHEST, preferred_element_type=jnp.float32)
    return jnp.concatenate(tendency, axis=0)


def reference(bin_state, courant_x, courant_y, cloudy_order, block_count, gain_kernel, loss_rate):
    state_now = bin_state
    serial = jnp.arange(N_GX * MEANB, dtype=jnp.int32)
    for step_index in range(STEPS):
        state_now = lax.map(lambda component: transport(component, courant_x, courant_y), state_now)
        current = state_now

        def row_tendency(row_index):
            counts_row = block_count[row_index].astype(jnp.int32)
            count_ends = jnp.cumsum(counts_row).astype(jnp.int32)
            starts = (count_ends - counts_row).astype(jnp.int32)
            sender = jnp.sum((count_ends[None, :] <= serial[:, None]).astype(jnp.int32), axis=1).astype(jnp.int32)
            within = (serial - starts[sender]).astype(jnp.int32)
            local_block = cloudy_order[sender, row_index, within].astype(jnp.int32)
            global_row = (sender * CX + local_block).astype(jnp.int32)
            row_cells = lax.dynamic_slice_in_dim(current, (row_index * BLOCK).astype(jnp.int32), BLOCK, 2)
            chosen = jnp.take(row_cells, global_row, axis=1).astype(jnp.bfloat16)
            result = collide(chosen.reshape(COMPS, N_GX * MEANB * BLOCK), gain_kernel, loss_rate).astype(jnp.bfloat16)
            result = result.reshape(COMPS, N_GX * MEANB, BLOCK)
            return jnp.zeros((COMPS, NX, BLOCK), jnp.bfloat16).at[:, global_row].set(result)

        gathered = lax.map(row_tendency, jnp.arange(N_GY, dtype=jnp.int32))
        gathered = jnp.transpose(gathered, (1, 2, 0, 3)).reshape(COMPS, NX, N_GY * BLOCK)
        state_now = state_now + gathered.astype(jnp.float32)
    return state_now
```

```python
import jax
import jax.numpy as jnp
import numpy as np
from jax import lax
from jax.experimental import pallas as pl
from jax.experimental.pallas import tpu as pltpu
from jax.sharding import PartitionSpec as P

BINS = 33
COMPS = 132
ROWS = 136
PACKED = 144
LEV = 4
CX = 8
LANES = 128
HALF = 512
FLAT = BINS * BINS
WIDE = 1152
MESH = pl.DeviceIdType.MESH
F32, BF16 = jnp.float32, jnp.bfloat16

OFFSET = (0, 33, 66, 128)
STACK = (3, 6, 8, 5, 0, 1, 2, 4, 7, 9)
SWAPPED = 4
PLACE = {p: s for s, p in enumerate(STACK)}
GROUPS = (
    (1, 0, ((0, 0), (1, 1))),
    (1, 1, ((4, 1),)),
    (2, 0, ((2, 2),)),
    (3, 2, ((5, 1), (7, 2))),
    (3, 3, ((3, 0), (6, 1), (8, 2), (9, 3))),
)
PAIR_OF = {(0, 0): 0, (0, 1): 1, (0, 2): 2, (0, 3): 3, (1, 1): 4, (1, 2): 5, (1, 3): 6, (2, 2): 7, (2, 3): 8, (3, 3): 9}
CHUNK = 11
SLAB = BINS * 32


def iota(shape, dim):
    return lax.broadcasted_iota(jnp.int32, shape, dim)


def stack_gain(gain, stacked):
    stacked[...] = jnp.zeros_like(stacked)
    for place, pair in enumerate(STACK):
        stacked[place * 48 : place * 48 + BINS, 0:FLAT] = gain[pair]


def exchange(stacked, chooser):
    rows = SWAPPED * 48
    source = stacked[0:rows, :]
    width = 384
    parts = []
    for part in range(WIDE // width):
        column = iota((1, width), 1) + part * width
        high = (column * 1986) >> 16
        origin = jnp.where(column < FLAT, (column - high * BINS) * BINS + high, -1)
        chooser[...] = jnp.where(iota((WIDE, width), 0) == origin, 1.0, 0.0).astype(BF16)
        parts.append(
            jnp.dot(source, chooser[...], preferred_element_type=F32).astype(BF16)
        )
    for part in range(WIDE // width):
        stacked[0:rows, part * width : (part + 1) * width] = parts[part]


def window(stacked, pair, index, lane0):
    row = PLACE[pair] * 48
    start = index * BINS
    tile, off = start // LANES, start % LANES
    shift = (lane0 - off) % LANES
    def moved(t):
        value = stacked[row : row + 48, t * LANES : (t + 1) * LANES]
        return pltpu.roll(value, shift, 1) if shift else value
    first = moved(tile)
    if off + BINS <= LANES:
        return first
    return jnp.where(iota((48, LANES), 1) < lane0 + LANES - off, first, moved(tile + 1))


def build_gain(stacked, matrix, corner, corner2):
    lane = iota((48, LANES), 1)
    corner[...] = jnp.zeros_like(corner)
    corner2[...] = jnp.zeros_like(corner2)
    for group, (target, factor, pairs) in enumerate(GROUPS):
        for index in range(BINS):
            low, high = None, None
            for pair, cls in sorted(pairs, key=lambda entry: entry[1]):
                lane0 = OFFSET[cls] % LANES
                piece = window(stacked, pair, index, lane0)
                inside = (lane >= lane0) & (lane < lane0 + BINS)
                if cls == 3:
                    high = jnp.where(inside, piece, jnp.zeros_like(piece))
                else:
                    low = jnp.where(inside, piece, jnp.zeros_like(piece) if low is None else low)
            row = group * SLAB + index * 32
            for value, col in ((low, 0), (high, LANES)):
                if value is None:
                    continue
                matrix[row : row + 32, col : col + LANES] = value[0:32]
                last = value[32:48].astype(F32)[0:1]
                if target == 2:
                    corner2[index : index + 1, :] = last
                else:
                    at = factor * BINS + index
                    corner[at : at + 1, col : col + LANES] = last


def build_loss(loss, square, table):
    table[...] = jnp.zeros_like(table)
    square[...] = jnp.zeros_like(square)
    for (a, b), pair in PAIR_OF.items():
        square[0:BINS, 0:BINS] = loss[pair].astype(F32)
        plain = square[...]
        turned = plain.T
        if a == b:
            plain = plain + turned
        table[a * BINS : a * BINS + BINS, OFFSET[b] : OFFSET[b] + BINS] = plain[0:BINS, 0:BINS]
        if a != b:
            table[b * BINS : b * BINS + BINS, OFFSET[a] : OFFSET[a] + BINS] = turned[0:BINS, 0:BINS]


def build_weights(cx, cy, weights):
    own = jnp.ones((CX, LANES), F32)
    for axis, ref in enumerate((cx, cy)):
        c = ref[...]
        up = c > 0.0
        weights[axis * 4 + 0] = c * jnp.where(up, 1.0 / 3.0, 1.0)
        weights[axis * 4 + 1] = c * jnp.where(up, 0.0, -1.0 / 6.0)
        weights[axis * 4 + 2] = c * jnp.where(up, -1.0, -1.0 / 3.0)
        weights[axis * 4 + 3] = c * jnp.where(up, 1.0 / 6.0, 0.0)
        own = own - c * jnp.where(up, 0.5, -0.5)
    weights[8] = own


def pack_y(wide, ys):
    ys[...] = jnp.zeros_like(ys)
    for row in range(0, ROWS, 16):
        n = min(16, ROWS - row)
        lane = iota((n, LANES), 1)
        left = jnp.zeros((n, LANES), F32)
        right = jnp.zeros((n, LANES), F32)
        for b in range(CX):
            value = wide[b + 2, row : row + n, :]
            inside = (lane >= 8 * b) & (lane < 8 * b + 8)
            left = jnp.where(inside, pltpu.roll(value, 8 * b, 1) if b else value, left)
            right = jnp.where(inside, pltpu.roll(value, (8 * b + 8) % LANES, 1), right)
        ys[0, row : row + n, :] = left.astype(BF16)
        ys[1, row : row + n, :] = right.astype(BF16)


def transport(wide, left, right, weights, moved, cells, cells16):
    def block(pos, carry):
        b = (pos + 6) % 8
        half, col = pos // 4, pl.multiple_of((pos % 4) * LANES, LANES)
        w = [weights[k, pl.ds(b, 1), :] for k in range(9)]
        back = (120 - 8 * b) % LANES
        fore = (LANES - 8 * b) % LANES
        for row in range(0, ROWS, 16):
            n = min(16, ROWS - row)
            lane = iota((n, LANES), 1)
            rows = slice(row, row + n)
            q = wide[b + 2, rows, :]
            total = w[8] * q
            total = total - w[0] * wide[b + 3, rows, :] - w[1] * wide[b + 4, rows, :]
            total = total - w[2] * wide[b + 1, rows, :] - w[3] * wide[b, rows, :]
            before = pltpu.roll(left[rows, :].astype(F32), back, 1)
            after = pltpu.roll(right[rows, :].astype(F32), fore, 1)
            total = total - w[4] * pltpu.roll(jnp.where(lane < LEV, after, q), LANES - LEV, 1)
            total = total - w[5] * pltpu.roll(jnp.where(lane < 2 * LEV, after, q), LANES - 2 * LEV, 1)
            total = total - w[6] * pltpu.roll(jnp.where(lane >= LANES - LEV, before, q), LEV, 1)
            total = total - w[7] * pltpu.roll(jnp.where(lane >= LANES - 2 * LEV, before, q), 2 * LEV, 1)
            total = jnp.maximum(total, 0.0)
            moved[b, rows, :] = total
            rounded = total.astype(BF16)
            cells[half, rows, pl.ds(col, LANES)] = rounded.astype(F32)
            if row < 96:
                cells16[half, rows, pl.ds(col, LANES)] = rounded
            elif row == 96:
                kept = jnp.where(iota((n, LANES), 0) < 3, total, 0.0)
                cells16[half, rows, pl.ds(col, LANES)] = kept.astype(BF16)
        cells16[half, 128:176, pl.ds(col, LANES)] = cells[half, 99:147, pl.ds(col, LANES)].astype(BF16)
        return carry

    lax.fori_loop(0, CX, block, 0)


def collide(half, matrix, corner16, table16, moved, cells, cells16, gained, cloudy, put):
    total = {}
    for group, (target, factor, pairs) in enumerate(GROUPS):
        depth = 256 if any(cls == 3 for _, cls in pairs) else 128
        for first in range(0, BINS, CHUNK):
            row = group * SLAB + first * 32
            part = jnp.dot(
                matrix[row : row + CHUNK * 32, 0:depth],
                cells16[half, 0:depth, :],
                preferred_element_type=F32,
            )
            for k in range(CHUNK):
                at = factor * BINS + first + k
                term = cells[half, at : at + 1, :] * part[32 * k : 32 * k + 32]
                total[target] = total[target] + term if target in total else term
    for target in (1, 2, 3):
        gained[target * BINS : target * BINS + 32, :] = total[target]
    last = jnp.dot(corner16[...], cells16[half], preferred_element_type=F32)
    ends = last[0:ROWS] * cells[half, 0:ROWS, :]
    below = iota((ROWS, HALF), 0) < 2 * BINS
    gained[65:66, :] = jnp.sum(jnp.where(below, ends, 0.0), axis=0, keepdims=True)
    gained[131:132, :] = jnp.sum(jnp.where(below, 0.0, ends), axis=0, keepdims=True)
    second = last[PACKED : PACKED + 40] * cells[half, 0:40, :]
    gained[98:99, :] = jnp.sum(second, axis=0, keepdims=True)
    lost = jnp.dot(table16[...], cells16[half], preferred_element_type=F32)
    for pos in range(4):
        b = (4 * half + pos + 6) % 8
        col = slice(pos * LANES, (pos + 1) * LANES)
        share = cloudy[b]
        for row in range(0, ROWS, 8):
            rows = slice(row, row + 8)
            change = gained[rows, col] - cells[half, rows, col] * lost[rows, col]
            change = change.astype(BF16).astype(F32) * share
            put(b, row, moved[b, rows, :] + change)


def kernel(
    state, cx, cy, order, count, gain, loss, out,
    wide, moved, cells, cells16, stacked, chooser, matrix, corner, corner16, square, table, table16,
    gained, weights, cloudy, xs, ys, xr, yr, send_sem, recv_sem,
):
    gx, gy = lax.axis_index("gx"), lax.axis_index("gy")
    nx, ny = lax.axis_size("gx"), lax.axis_size("gy")
    peers = (
        (lax.rem(gx + nx - 1, nx), gy),
        (lax.rem(gx + 1, nx), gy),
        (gx, lax.rem(gy + ny - 1, ny)),
        (gx, lax.rem(gy + 1, ny)),
    )
    barrier = pltpu.get_barrier_semaphore()
    for peer in peers:
        pl.semaphore_signal(barrier, inc=1, device_id=peer, device_id_type=MESH)

    def copy(step, side):
        sent, kept = (xs, xr) if side < 2 else (ys, yr)
        return pltpu.make_async_remote_copy(
            src_ref=sent.at[step, side % 2],
            dst_ref=kept.at[step, side % 2],
            send_sem=send_sem.at[step, side],
            recv_sem=recv_sem.at[step, side],
            device_id=peers[side],
            device_id_type=MESH,
        )

    def pack_x(step, side):
        for column in range(2):
            xs[step, side, column, 0:ROWS, :] = wide[2 + 6 * side + column].astype(BF16)

    for b in range(CX):
        for row in range(0, COMPS, 8):
            n = min(8, COMPS - row)
            wide[b + 2, row : row + n, :] = state[pl.ds(row * CX + b, n, stride=CX), :]
        wide[b + 2, COMPS:ROWS, :] = jnp.zeros((ROWS - COMPS, LANES), F32)
    for side in range(2):
        for step in range(2):
            for column in range(2):
                xs[step, side, column, ROWS - 8 :, :] = jnp.zeros((PACKED - ROWS + 8, LANES), BF16)
        pack_x(0, side)
    pack_y(wide, ys.at[0])
    pl.semaphore_wait(barrier, 4)
    for side in range(4):
        copy(0, side).start()

    cells[...] = jnp.zeros_like(cells)
    cells16[...] = jnp.zeros_like(cells16)
    gained[0:40, :] = jnp.zeros((40, HALF), F32)
    gained[ROWS - 8 :, :] = jnp.zeros((8, HALF), F32)
    for b in range(CX):
        found = jnp.int32(0)
        for k in range(CX):
            hit = (order[0, 0, k] == b) & (k < count[0, 0])
            found = found + hit.astype(jnp.int32)
        cloudy[b] = found.astype(F32)
    build_weights(cx, cy, weights)
    stack_gain(gain, stacked)
    exchange(stacked, chooser)
    build_gain(stacked, matrix, corner, corner.at[PACKED : PACKED + 48, 0:LANES])
    build_loss(loss, square, table)
    corner16[...] = corner[...].astype(BF16)
    table16[...] = table[...].astype(BF16)

    for step in range(2):
        for side in range(4):
            copy(step, side).wait_recv()
        for column in range(2):
            wide[column] = xr[step, 1, column, 0:ROWS, :].astype(F32)
            wide[CX + 2 + column] = xr[step, 0, column, 0:ROWS, :].astype(F32)
        transport(wide, yr.at[step, 1], yr.at[step, 0], weights, moved, cells, cells16)

        def put(b, row, value):
            if step == 0:
                wide[b + 2, row : row + 8, :] = value
            else:
                n = min(8, COMPS - row)
                out[pl.ds(row * CX + b, n, stride=CX), :] = value[0:n]

        for half in range(2):
            collide(half, matrix, corner16, table16, moved, cells, cells16, gained, cloudy, put)
            if step == 0 and half == 0:
                for side in range(2):
                    pack_x(1, side)
                for side in range(2):
                    copy(1, side).start()
        if step == 0:
            pack_y(wide, ys.at[1])
            for side in range(2, 4):
                copy(1, side).start()
    for step in range(2):
        for side in range(4):
            copy(step, side).wait_send()


def per_device(bin_state, courant_x, courant_y, cloudy_order, block_count, gain_kernel, loss_rate):
    vmem = pl.BlockSpec(memory_space=pltpu.VMEM)
    smem = pl.BlockSpec(memory_space=pltpu.SMEM)
    flat = bin_state.reshape(COMPS * CX, LANES)
    result = pl.pallas_call(
        kernel,
        out_shape=jax.ShapeDtypeStruct(flat.shape, F32),
        in_specs=[vmem, vmem, vmem, smem, smem, vmem, vmem],
        out_specs=vmem,
        scratch_shapes=[
            pltpu.VMEM((CX + 4, ROWS, LANES), F32),
            pltpu.VMEM((CX, ROWS, LANES), F32),
            pltpu.VMEM((2, 152, HALF), F32),
            pltpu.VMEM((2, 256, HALF), BF16),
            pltpu.VMEM((480, WIDE), BF16),
            pltpu.VMEM((WIDE, 384), BF16),
            pltpu.VMEM((len(GROUPS) * SLAB, 256), BF16),
            pltpu.VMEM((PACKED + 48, 256), F32),
            pltpu.VMEM((PACKED + 48, 256), BF16),
            pltpu.VMEM((LANES, LANES), F32),
            pltpu.VMEM((PACKED, 256), F32),
            pltpu.VMEM((PACKED, 256), BF16),
            pltpu.VMEM((ROWS, HALF), F32),
            pltpu.VMEM((9, CX, LANES), F32),
            pltpu.SMEM((CX,), F32),
            pltpu.VMEM((2, 2, 2, PACKED, LANES), BF16),
            pltpu.VMEM((2, 2, PACKED, LANES), BF16),
            pltpu.VMEM((2, 2, 2, PACKED, LANES), BF16),
            pltpu.VMEM((2, 2, PACKED, LANES), BF16),
            pltpu.SemaphoreType.DMA((2, 4)),
            pltpu.SemaphoreType.DMA((2, 4)),
        ],
        compiler_params=pltpu.CompilerParams(collective_id=0, has_side_effects=True),
        name="microphysics",
    )(flat, courant_x, courant_y, cloudy_order, block_count, gain_kernel, loss_rate)
    return result.reshape(bin_state.shape)


def solution(mesh):
    placed = (
        P(None, "gx", "gy"),
        P("gx", "gy"),
        P("gx", "gy"),
        P("gx", "gy", None),
        P("gy", "gx"),
        P(),
        P(),
    )
    return jax.shard_map(
        per_device, mesh=mesh, in_specs=placed, out_specs=P(None, "gx", "gy"), check_vma=False
    )
```

```python
import jax
import jax.numpy as jnp
import numpy as np
from jax import lax
from jax.experimental import pallas as pl
from jax.experimental.pallas import tpu as pltpu
from jax.sharding import PartitionSpec as P

BINS = 33
COMPS = 132
ROWS = 136
PACKED = 144
LEV = 4
CX = 8
LANES = 128
HALF = 512
FLAT = BINS * BINS
WIDE = 1152
MESH = pl.DeviceIdType.MESH
F32, BF16 = jnp.float32, jnp.bfloat16

OFFSET = (0, 33, 66, 128)
STACK = (3, 6, 8, 5, 0, 1, 2, 4, 7, 9)
SWAPPED = 4
PLACE = {p: s for s, p in enumerate(STACK)}
GROUPS = (
    (1, 0, ((0, 0), (1, 1))),
    (1, 1, ((4, 1),)),
    (2, 0, ((2, 2),)),
    (3, 2, ((5, 1), (7, 2))),
    (3, 3, ((3, 0), (6, 1), (8, 2), (9, 3))),
)
PAIR_OF = {(0, 0): 0, (0, 1): 1, (0, 2): 2, (0, 3): 3, (1, 1): 4, (1, 2): 5, (1, 3): 6, (2, 2): 7, (2, 3): 8, (3, 3): 9}
CHUNK = 11
SLAB = BINS * 32


def iota(shape, dim):
    return lax.broadcasted_iota(jnp.int32, shape, dim)


def stack_gain(gain, stacked):
    stacked[...] = jnp.zeros_like(stacked)
    for place, pair in enumerate(STACK):
        stacked[place * 48 : place * 48 + BINS, 0:FLAT] = gain[pair]


def exchange(stacked, chooser):
    rows = SWAPPED * 48
    source = stacked[0:rows, :]
    width = 384
    parts = []
    for part in range(WIDE // width):
        column = iota((1, width), 1) + part * width
        high = (column * 1986) >> 16
        origin = jnp.where(column < FLAT, (column - high * BINS) * BINS + high, -1)
        chooser[...] = jnp.where(iota((WIDE, width), 0) == origin, 1.0, 0.0).astype(BF16)
        parts.append(
            jnp.dot(source, chooser[...], preferred_element_type=F32).astype(BF16)
        )
    for part in range(WIDE // width):
        stacked[0:rows, part * width : (part + 1) * width] = parts[part]


def window(stacked, pair, index, lane0):
    row = PLACE[pair] * 48
    start = index * BINS
    tile, off = start // LANES, start % LANES
    shift = (lane0 - off) % LANES
    def moved(t):
        value = stacked[row : row + 48, t * LANES : (t + 1) * LANES]
        return pltpu.roll(value, shift, 1) if shift else value
    first = moved(tile)
    if off + BINS <= LANES:
        return first
    return jnp.where(iota((48, LANES), 1) < lane0 + LANES - off, first, moved(tile + 1))


def build_gain(stacked, matrix, corner, corner2):
    lane = iota((48, LANES), 1)
    corner[...] = jnp.zeros_like(corner)
    corner2[...] = jnp.zeros_like(corner2)
    for group, (target, factor, pairs) in enumerate(GROUPS):
        for index in range(BINS):
            low, high = None, None
            for pair, cls in sorted(pairs, key=lambda entry: entry[1]):
                lane0 = OFFSET[cls] % LANES
                piece = window(stacked, pair, index, lane0)
                inside = (lane >= lane0) & (lane < lane0 + BINS)
                if cls == 3:
                    high = jnp.where(inside, piece, jnp.zeros_like(piece))
                else:
                    low = jnp.where(inside, piece, jnp.zeros_like(piece) if low is None else low)
            row = group * SLAB + index * 32
            for value, col in ((low, 0), (high, LANES)):
                if value is None:
                    continue
                matrix[row : row + 32, col : col + LANES] = value[0:32]
                last = value[32:48].astype(F32)[0:1]
                if target == 2:
                    corner2[index : index + 1, :] = last
                else:
                    at = factor * BINS + index
                    corner[at : at + 1, col : col + LANES] = last


def build_loss(loss, square, table):
    table[...] = jnp.zeros_like(table)
    square[...] = jnp.zeros_like(square)
    for (a, b), pair in PAIR_OF.items():
        square[0:BINS, 0:BINS] = loss[pair].astype(F32)
        plain = square[...]
        turned = plain.T
        if a == b:
            plain = plain + turned
        table[a * BINS : a * BINS + BINS, OFFSET[b] : OFFSET[b] + BINS] = plain[0:BINS, 0:BINS]
        if a != b:
            table[b * BINS : b * BINS + BINS, OFFSET[a] : OFFSET[a] + BINS] = turned[0:BINS, 0:BINS]


def build_weights(cx, cy, weights):
    own = jnp.ones((CX, LANES), F32)
    for axis, ref in enumerate((cx, cy)):
        c = ref[...]
        up = c > 0.0
        weights[axis * 4 + 0] = c * jnp.where(up, 1.0 / 3.0, 1.0)
        weights[axis * 4 + 1] = c * jnp.where(up, 0.0, -1.0 / 6.0)
        weights[axis * 4 + 2] = c * jnp.where(up, -1.0, -1.0 / 3.0)
        weights[axis * 4 + 3] = c * jnp.where(up, 1.0 / 6.0, 0.0)
        own = own - c * jnp.where(up, 0.5, -0.5)
    weights[8] = own


def build_bands(weights, bands):
    def block(b, carry):
        row, lane = iota((LANES, LANES), 0), iota((LANES, LANES), 1)
        left, right = row - 8 * b, row - 64 - 8 * b
        far = jnp.full_like(row, -1000)
        outer = jnp.where((left >= 0) & (left < 8), left - 8, far)
        outer = jnp.where((right >= 0) & (right < 8), right + LANES, outer)
        for part, place in ((0, row), (1, outer)):
            value = jnp.zeros((LANES, LANES), F32)
            for k, shift in ((4, LEV), (5, 2 * LEV), (6, -LEV), (7, -2 * LEV)):
                value = jnp.where(place - lane == shift, -weights[k, pl.ds(b, 1), :], value)
            bands[b, part * LANES : (part + 1) * LANES, :] = value.astype(BF16)
        return carry

    lax.fori_loop(0, CX, block, 0)


def pack_y(narrow, ys):
    lane = iota((16, LANES), 1)
    for row in range(0, PACKED, 16):
        left = jnp.zeros((16, LANES), BF16)
        right = jnp.zeros((16, LANES), BF16)
        for b in range(CX):
            value = narrow[b, row : row + 16, 0:LANES]
            at = 64 + 8 * b
            left = jnp.where((lane >= at) & (lane < at + 8), pltpu.roll(value, at, 1), left)
            at = 8 * b
            right = jnp.where((lane >= at) & (lane < at + 8), pltpu.roll(value, at + 8, 1), right)
        ys[0, row : row + 16, :] = left
        ys[1, row : row + 16, :] = right


def transport(wide, narrow, bands, weights, moved, cells, cells16):
    for pos in range(CX):
        b = (pos + 6) % 8
        half, cols = pos // 4, slice((pos % 4) * LANES, (pos % 4 + 1) * LANES)
        w = [weights[k, b : b + 1, :] for k in (0, 1, 2, 3, 8)]
        flux = jnp.dot(narrow[b], bands[b], preferred_element_type=F32)
        for row in range(0, ROWS, 16):
            n = min(16, ROWS - row)
            rows = slice(row, row + n)
            total = w[4] * wide[b + 2, rows, :] + flux[rows]
            total = total - w[0] * wide[b + 3, rows, :] - w[1] * wide[b + 4, rows, :]
            total = total - w[2] * wide[b + 1, rows, :] - w[3] * wide[b, rows, :]
            total = jnp.maximum(total, 0.0)
            moved[b, rows, :] = total
            rounded = total.astype(BF16)
            cells[half, rows, cols] = rounded.astype(F32)
            if row < 96:
                cells16[half, rows, cols] = rounded
            elif row == 96:
                kept = jnp.where(iota((n, LANES), 0) < 3, total, 0.0)
                cells16[half, rows, cols] = kept.astype(BF16)
        cells16[half, 128:176, cols] = cells[half, 99:147, cols].astype(BF16)


def collide(half, matrix, corner16, table16, moved, cells, cells16, gained, cloudy, put):
    total = {}
    for group, (target, factor, pairs) in enumerate(GROUPS):
        depth = 256 if any(cls == 3 for _, cls in pairs) else 128
        for first in range(0, BINS, CHUNK):
            row = group * SLAB + first * 32
            part = jnp.dot(
                matrix[row : row + CHUNK * 32, 0:depth],
                cells16[half, 0:depth, :],
                preferred_element_type=F32,
            )
            for k in range(CHUNK):
                at = factor * BINS + first + k
                term = cells[half, at : at + 1, :] * part[32 * k : 32 * k + 32]
                total[target] = total[target] + term if target in total else term
    for target in (1, 2, 3):
        gained[target * BINS : target * BINS + 32, :] = total[target]
    last = jnp.dot(corner16[...], cells16[half], preferred_element_type=F32)
    ends = last[0:ROWS] * cells[half, 0:ROWS, :]
    below = iota((ROWS, HALF), 0) < 2 * BINS
    gained[65:66, :] = jnp.sum(jnp.where(below, ends, 0.0), axis=0, keepdims=True)
    gained[131:132, :] = jnp.sum(jnp.where(below, 0.0, ends), axis=0, keepdims=True)
    second = last[PACKED : PACKED + 40] * cells[half, 0:40, :]
    gained[98:99, :] = jnp.sum(second, axis=0, keepdims=True)
    lost = jnp.dot(table16[...], cells16[half], preferred_element_type=F32)
    for pos in range(4):
        b = (4 * half + pos + 6) % 8
        col = slice(pos * LANES, (pos + 1) * LANES)
        share = cloudy[b]
        for row in range(0, ROWS, 16):
            rows = slice(row, min(row + 16, ROWS))
            change = gained[rows, col] - cells[half, rows, col] * lost[rows, col]
            change = change.astype(BF16).astype(F32) * share
            put(b, row, moved[b, rows, :] + change)


def kernel(
    state_hbm, cx_hbm, cy_hbm, order_hbm, count, gain_hbm, loss_hbm, out,
    state, cx, cy, order, gain, loss,
    wide, narrow, moved, cells, cells16, stacked, chooser, matrix, corner, corner16, square, table, table16,
    gained, weights, bands, cloudy, xs, ys, xr, yr, load_sem, send_sem, recv_sem,
):
    gx, gy = lax.axis_index("gx"), lax.axis_index("gy")
    nx, ny = lax.axis_size("gx"), lax.axis_size("gy")
    peers = (
        (lax.rem(gx + nx - 1, nx), gy),
        (lax.rem(gx + 1, nx), gy),
        (gx, lax.rem(gy + ny - 1, ny)),
        (gx, lax.rem(gy + 1, ny)),
    )
    loads = [
        pltpu.make_async_copy(source, kept, load_sem.at[k])
        for k, (source, kept) in enumerate(
            (
                (state_hbm, state), (cx_hbm, cx), (cy_hbm, cy), (order_hbm, order),
                (gain_hbm, gain), (loss_hbm, loss),
            )
        )
    ]
    for load in loads:
        load.start()
    barrier = pltpu.get_barrier_semaphore()
    for peer in peers:
        pl.semaphore_signal(barrier, inc=1, device_id=peer, device_id_type=MESH)

    def copy(step, side):
        sent, kept = (xs, xr) if side < 2 else (ys, yr)
        return pltpu.make_async_remote_copy(
            src_ref=sent.at[step, side % 2],
            dst_ref=kept.at[step, side % 2],
            send_sem=send_sem.at[step, side],
            recv_sem=recv_sem.at[step, side],
            device_id=peers[side],
            device_id_type=MESH,
        )

    def pack_x(step):
        for side in range(2):
            for column in range(2):
                xs[step, side, column] = narrow[6 * side + column, :, 0:LANES]

    for b in range(CX):
        wide[b + 2, 128:ROWS, :] = jnp.zeros((ROWS - 128, LANES), F32)
        narrow[b, 128:PACKED, 0:LANES] = jnp.zeros((PACKED - 128, LANES), BF16)
    loads[0].wait()
    for b in range(CX):
        for row in range(0, 128, 16):
            value = state[pl.ds(row * CX + b, 16, stride=CX), :]
            wide[b + 2, row : row + 16, :] = value
            narrow[b, row : row + 16, 0:LANES] = value.astype(BF16)
        value = state[pl.ds(128 * CX + b, COMPS - 128, stride=CX), :]
        wide[b + 2, 128:COMPS, :] = value
        narrow[b, 128:ROWS, 0:LANES] = wide[b + 2, 128:ROWS, :].astype(BF16)
    pack_y(narrow, ys.at[0])
    pack_x(0)
    pl.semaphore_wait(barrier, 4)
    for side in (2, 3, 0, 1):
        copy(0, side).start()

    cells[...] = jnp.zeros_like(cells)
    cells16[...] = jnp.zeros_like(cells16)
    gained[0:40, :] = jnp.zeros((40, HALF), F32)
    gained[ROWS - 8 :, :] = jnp.zeros((8, HALF), F32)
    for load in loads[1:]:
        load.wait()
    for b in range(CX):
        found = jnp.int32(0)
        for k in range(CX):
            hit = (order[0, 0, k] == b) & (k < count[0, 0])
            found = found + hit.astype(jnp.int32)
        cloudy[b] = found.astype(F32)
    build_weights(cx, cy, weights)
    build_bands(weights, bands)
    stack_gain(gain, stacked)
    exchange(stacked, chooser)
    build_gain(stacked, matrix, corner, corner.at[PACKED : PACKED + 48, 0:LANES])
    build_loss(loss, square, table)
    corner16[...] = corner[...].astype(BF16)
    table16[...] = table[...].astype(BF16)

    for step in range(2):
        for side in range(4):
            copy(step, side).wait_recv()
        for column in range(2):
            wide[column] = xr[step, 1, column, 0:ROWS, :].astype(F32)
            wide[CX + 2 + column] = xr[step, 0, column, 0:ROWS, :].astype(F32)
        halo = yr[step, 0] + yr[step, 1]
        for b in range(CX):
            narrow[b, :, LANES : 2 * LANES] = halo
        transport(wide, narrow, bands, weights, moved, cells, cells16)

        def put(b, row, value):
            if step == 0:
                n = value.shape[0]
                wide[b + 2, row : row + n, :] = value
                narrow[b, row : row + n, 0:LANES] = value.astype(BF16)
            else:
                n = min(16, COMPS - row)
                out[pl.ds(row * CX + b, n, stride=CX), :] = value[0:n]

        for half in range(2):
            collide(half, matrix, corner16, table16, moved, cells, cells16, gained, cloudy, put)
            if step == 0 and half == 0:
                pack_x(1)
                for side in range(2):
                    copy(1, side).start()
        if step == 0:
            pack_y(narrow, ys.at[1])
            for side in range(2, 4):
                copy(1, side).start()
    for step in range(2):
        for side in range(4):
            copy(step, side).wait_send()


def pinned(array):
    return pltpu.with_memory_space_constraint(array, pltpu.HBM)


def per_device(bin_state, courant_x, courant_y, cloudy_order, block_count, gain_kernel, loss_rate):
    vmem = pl.BlockSpec(memory_space=pltpu.VMEM)
    hbm = pl.BlockSpec(memory_space=pltpu.HBM)
    flat = bin_state.reshape(COMPS * CX, LANES)
    result = pl.pallas_call(
        kernel,
        out_shape=jax.ShapeDtypeStruct(flat.shape, F32),
        in_specs=[hbm] * 4 + [pl.BlockSpec(memory_space=pltpu.VMEM)] + [hbm] * 2,
        out_specs=vmem,
        scratch_shapes=[
            pltpu.VMEM(flat.shape, F32),
            pltpu.VMEM(courant_x.shape, F32),
            pltpu.VMEM(courant_y.shape, F32),
            pltpu.SMEM(cloudy_order.shape, jnp.int32),
            pltpu.VMEM(gain_kernel.shape, BF16),
            pltpu.VMEM(loss_rate.shape, BF16),
            pltpu.VMEM((CX + 4, ROWS, LANES), F32),
            pltpu.VMEM((CX, PACKED, 2 * LANES), BF16),
            pltpu.VMEM((CX, ROWS, LANES), F32),
            pltpu.VMEM((2, 152, HALF), F32),
            pltpu.VMEM((2, 256, HALF), BF16),
            pltpu.VMEM((480, WIDE), BF16),
            pltpu.VMEM((WIDE, 384), BF16),
            pltpu.VMEM((len(GROUPS) * SLAB, 256), BF16),
            pltpu.VMEM((PACKED + 48, 256), F32),
            pltpu.VMEM((PACKED + 48, 256), BF16),
            pltpu.VMEM((LANES, LANES), F32),
            pltpu.VMEM((PACKED, 256), F32),
            pltpu.VMEM((PACKED, 256), BF16),
            pltpu.VMEM((ROWS, HALF), F32),
            pltpu.VMEM((9, CX, LANES), F32),
            pltpu.VMEM((CX, 2 * LANES, LANES), BF16),
            pltpu.SMEM((CX,), F32),
            pltpu.VMEM((2, 2, 2, PACKED, LANES), BF16),
            pltpu.VMEM((2, 2, PACKED, LANES), BF16),
            pltpu.VMEM((2, 2, 2, PACKED, LANES), BF16),
            pltpu.VMEM((2, 2, PACKED, LANES), BF16),
            pltpu.SemaphoreType.DMA((6,)),
            pltpu.SemaphoreType.DMA((2, 4)),
            pltpu.SemaphoreType.DMA((2, 4)),
        ],
        compiler_params=pltpu.CompilerParams(
            collective_id=0, has_side_effects=True, vmem_limit_bytes=24 * 1024 * 1024
        ),
        name="microphysics",
    )(
        pinned(flat), pinned(courant_x), pinned(courant_y), pinned(cloudy_order), block_count,
        pinned(gain_kernel), pinned(loss_rate),
    )
    return result.reshape(bin_state.shape)


def solution(mesh):
    placed = (
        P(None, "gx", "gy"),
        P("gx", "gy"),
        P("gx", "gy"),
        P("gx", "gy", None),
        P("gy", "gx"),
        P(),
        P(),
    )
    return jax.shard_map(
        per_device, mesh=mesh, in_specs=placed, out_specs=P(None, "gx", "gy"), check_vma=False
    )
```

```python
import jax
import jax.numpy as jnp
import numpy as np
from jax import lax
from jax.experimental import pallas as pl
from jax.experimental.pallas import tpu as pltpu
from jax.sharding import PartitionSpec as P

BINS = 33
COMPS = 132
ROWS = 136
PACKED = 144
LEV = 4
CX = 8
LANES = 128
HALF = 512
FLAT = BINS * BINS
WIDE = 1152
MESH = pl.DeviceIdType.MESH
F32, BF16 = jnp.float32, jnp.bfloat16

OFFSET = (0, 33, 66, 128)
STACK = (3, 6, 8, 5, 0, 1, 2, 4, 7, 9)
SWAPPED = 4
PLACE = {p: s for s, p in enumerate(STACK)}
GROUPS = (
    (1, 0, ((0, 0), (1, 1))),
    (1, 1, ((4, 1),)),
    (2, 0, ((2, 2),)),
    (3, 2, ((5, 1), (7, 2))),
    (3, 3, ((3, 0), (6, 1), (8, 2), (9, 3))),
)
PAIR_OF = {(0, 0): 0, (0, 1): 1, (0, 2): 2, (0, 3): 3, (1, 1): 4, (1, 2): 5, (1, 3): 6, (2, 2): 7, (2, 3): 8, (3, 3): 9}
CHUNK = 11
SLAB = BINS * 32
PARTS = ((0, 48), (48, 48), (96, 40))


def iota(shape, dim):
    return lax.broadcasted_iota(jnp.int32, shape, dim)


def stack_gain(gain, stacked):
    stacked[...] = jnp.zeros_like(stacked)
    for place, pair in enumerate(STACK):
        stacked[place * 48 : place * 48 + BINS, 0:FLAT] = gain[pair]


def exchange(stacked, chooser):
    rows = SWAPPED * 48
    source = stacked[0:rows, :]
    width = 384
    parts = []
    for part in range(WIDE // width):
        column = iota((1, width), 1) + part * width
        high = (column * 1986) >> 16
        origin = jnp.where(column < FLAT, (column - high * BINS) * BINS + high, -1)
        chooser[...] = jnp.where(iota((WIDE, width), 0) == origin, 1.0, 0.0).astype(BF16)
        parts.append(
            jnp.dot(source, chooser[...], preferred_element_type=F32).astype(BF16)
        )
    for part in range(WIDE // width):
        stacked[0:rows, part * width : (part + 1) * width] = parts[part]


def window(stacked, lane, pair, index, lane0):
    row = PLACE[pair] * 48
    start = index * BINS
    tile, off = start // LANES, start % LANES
    shift = (lane0 - off) % LANES
    def moved(t):
        value = stacked[row : row + 48, t * LANES : (t + 1) * LANES]
        return pltpu.roll(value, shift, 1) if shift else value
    first = moved(tile)
    if off + BINS <= LANES:
        return first
    return jnp.where(lane < lane0 + LANES - off, first, moved(tile + 1))


def build_gain(stacked, matrix, corner, corner2):
    lane = iota((48, LANES), 1)
    inside = {at % LANES: (lane >= at % LANES) & (lane < at % LANES + BINS) for at in OFFSET}
    nothing = jnp.zeros((48, LANES), BF16)
    corner[...] = jnp.zeros_like(corner)
    corner2[...] = jnp.zeros_like(corner2)
    for group, (target, factor, pairs) in enumerate(GROUPS):
        for index in range(BINS):
            low, high = None, None
            for pair, cls in sorted(pairs, key=lambda entry: entry[1]):
                lane0 = OFFSET[cls] % LANES
                piece = window(stacked, lane, pair, index, lane0)
                if cls == 3:
                    high = jnp.where(inside[lane0], piece, nothing)
                else:
                    low = jnp.where(inside[lane0], piece, nothing if low is None else low)
            row = group * SLAB + index * 32
            for value, col in ((low, 0), (high, LANES)):
                if value is None:
                    continue
                matrix[row : row + 32, col : col + LANES] = value[0:32]
                last = value[32:48].astype(F32)[0:1]
                if target == 2:
                    corner2[index : index + 1, :] = last
                else:
                    at = factor * BINS + index
                    corner[at : at + 1, col : col + LANES] = last


def build_loss(loss, square, table):
    table[...] = jnp.zeros_like(table)
    square[...] = jnp.zeros_like(square)
    for (a, b), pair in PAIR_OF.items():
        square[0:BINS, 0:BINS] = loss[pair].astype(F32)
        plain = square[...]
        turned = plain.T
        if a == b:
            plain = plain + turned
        table[a * BINS : a * BINS + BINS, OFFSET[b] : OFFSET[b] + BINS] = plain[0:BINS, 0:BINS]
        if a != b:
            table[b * BINS : b * BINS + BINS, OFFSET[a] : OFFSET[a] + BINS] = turned[0:BINS, 0:BINS]


def build_weights(cx, cy, weights):
    own = jnp.ones((CX, LANES), F32)
    for axis, ref in enumerate((cx, cy)):
        c = ref[...]
        up = c > 0.0
        weights[axis * 4 + 0] = c * jnp.where(up, 1.0 / 3.0, 1.0)
        weights[axis * 4 + 1] = c * jnp.where(up, 0.0, -1.0 / 6.0)
        weights[axis * 4 + 2] = c * jnp.where(up, -1.0, -1.0 / 3.0)
        weights[axis * 4 + 3] = c * jnp.where(up, 1.0 / 6.0, 0.0)
        own = own - c * jnp.where(up, 0.5, -0.5)
    weights[8] = own


def build_bands(weights, bands):
    def block(b, carry):
        row, lane = iota((LANES, LANES), 0), iota((LANES, LANES), 1)
        left, right = row - 8 * b, row - 64 - 8 * b
        far = jnp.full_like(row, -1000)
        outer = jnp.where((left >= 0) & (left < 8), left - 8, far)
        outer = jnp.where((right >= 0) & (right < 8), right + LANES, outer)
        for part, place in ((0, row), (1, outer)):
            value = jnp.zeros((LANES, LANES), F32)
            for k, shift in ((4, LEV), (5, 2 * LEV), (6, -LEV), (7, -2 * LEV)):
                value = jnp.where(place - lane == shift, -weights[k, pl.ds(b, 1), :], value)
            bands[b, part * LANES : (part + 1) * LANES, :] = value.astype(BF16)
        return carry

    lax.fori_loop(0, CX, block, 0)


def edges(block, n, dtype):
    lane = iota((n, LANES), 1)
    total = jnp.zeros((n, LANES), dtype)
    for b in range(CX):
        value = block(b)
        for at, shift in ((8 * b, 8 * b + 8), (64 + 8 * b, 64 + 8 * b)):
            total = jnp.where((lane >= at) & (lane < at + 8), pltpu.roll(value, shift, 1), total)
    return total


def one_side(side, lane, total):
    return jnp.where(lane >= 64 if side == 0 else lane < 64, total, jnp.zeros_like(total))


def place(total, row, n, half, cells, cells16, cols):
    rows = slice(row, row + n)
    rounded = total.astype(BF16)
    cells[half, rows, cols] = rounded.astype(F32)
    if row < 96:
        cells16[half, rows, cols] = rounded
    else:
        kept = jnp.where(iota((16, LANES), 0) < 3, total[0:16], 0.0)
        cells16[half, 96:112, cols] = kept.astype(BF16)
        cells16[half, 128:176, cols] = cells[half, 99:147, cols].astype(BF16)


def transport(wide, narrow, bands, weights, moved, cells, cells16):
    for pos in range(CX):
        b = (pos + 6) % 8
        half, cols = pos // 4, slice((pos % 4) * LANES, (pos % 4 + 1) * LANES)
        w = [weights[k, b : b + 1, :] for k in (0, 1, 2, 3, 8)]
        flux = jnp.dot(narrow[b], bands[b], preferred_element_type=F32)
        for row, n in PARTS:
            rows = slice(row, row + n)
            total = w[4] * wide[b + 2, rows, :] + flux[rows]
            total = total - w[0] * wide[b + 3, rows, :] - w[1] * wide[b + 4, rows, :]
            total = total - w[2] * wide[b + 1, rows, :] - w[3] * wide[b, rows, :]
            total = jnp.maximum(total, 0.0)
            moved[b, rows, :] = total
            place(total, row, n, half, cells, cells16, cols)


def gather_edges(moved, edge, cells, cells16):
    for row, n in PARTS:
        total = edges(lambda b: moved[b, row : row + n, :], n, F32)
        edge[row : row + n, :] = total
        place(total, row, n, 0, cells, cells16, slice(0, LANES))


def collide(half, matrix, corner16, table16, cells, cells16, gained, finish):
    total, width = {}, cells.shape[2]
    for group, (target, factor, pairs) in enumerate(GROUPS):
        depth = 256 if any(cls == 3 for _, cls in pairs) else 128
        for first in range(0, BINS, CHUNK):
            row = group * SLAB + first * 32
            part = jnp.dot(
                matrix[row : row + CHUNK * 32, 0:depth],
                cells16[half, 0:depth, :],
                preferred_element_type=F32,
            )
            for k in range(CHUNK):
                at = factor * BINS + first + k
                term = cells[half, at : at + 1, :] * part[32 * k : 32 * k + 32]
                total[target] = total[target] + term if target in total else term
    for target in (1, 2, 3):
        gained[target * BINS : target * BINS + 32, :] = total[target]
    last = jnp.dot(corner16[...], cells16[half], preferred_element_type=F32)
    ends = last[0:ROWS] * cells[half, 0:ROWS, :]
    below = iota((ROWS, width), 0) < 2 * BINS
    gained[65:66, :] = jnp.sum(jnp.where(below, ends, 0.0), axis=0, keepdims=True)
    gained[131:132, :] = jnp.sum(jnp.where(below, 0.0, ends), axis=0, keepdims=True)
    second = last[PACKED : PACKED + 40] * cells[half, 0:40, :]
    gained[98:99, :] = jnp.sum(second, axis=0, keepdims=True)
    lost = jnp.dot(table16[...], cells16[half], preferred_element_type=F32)
    for pos in range(width // LANES):
        col = slice(pos * LANES, (pos + 1) * LANES)
        for row, n in PARTS:
            rows = slice(row, row + n)
            change = gained[rows, col] - cells[half, rows, col] * lost[rows, col]
            finish(pos, row, change.astype(BF16).astype(F32))


def kernel(
    state_hbm, cx_hbm, cy_hbm, order_hbm, count, gain_hbm, loss_hbm, out,
    state, cx, cy, order, gain, loss,
    wide, narrow, moved, cells, cells16, stacked, chooser, matrix, corner, corner16, square, table, table16,
    gained, weights, bands, cloudy, share, edge, edge_cells, edge_cells16, edge_gained, xs, ys, xr, yr, load_sem, send_sem, recv_sem,
):
    gx, gy = lax.axis_index("gx"), lax.axis_index("gy")
    nx, ny = lax.axis_size("gx"), lax.axis_size("gy")
    peers = (
        (lax.rem(gx + nx - 1, nx), gy),
        (lax.rem(gx + 1, nx), gy),
        (gx, lax.rem(gy + ny - 1, ny)),
        (gx, lax.rem(gy + 1, ny)),
    )
    loads = [
        pltpu.make_async_copy(source, kept, load_sem.at[k])
        for k, (source, kept) in enumerate(
            (
                (state_hbm, state), (cx_hbm, cx), (cy_hbm, cy), (order_hbm, order),
                (gain_hbm, gain), (loss_hbm, loss),
            )
        )
    ]
    for load in loads:
        load.start()
    barrier = pltpu.get_barrier_semaphore()
    for peer in peers:
        pl.semaphore_signal(barrier, inc=1, device_id=peer, device_id_type=MESH)

    def copy(step, side):
        sent, kept = (xs, xr) if side < 2 else (ys, yr)
        return pltpu.make_async_remote_copy(
            src_ref=sent.at[step, side % 2],
            dst_ref=kept.at[step, side % 2],
            send_sem=send_sem.at[step, side],
            recv_sem=recv_sem.at[step, side],
            device_id=peers[side],
            device_id_type=MESH,
        )

    def pack_x(step):
        for side in range(2):
            for column in range(2):
                xs[step, side, column] = narrow[6 * side + column, :, 0:LANES]

    for b in range(CX):
        wide[b + 2, 128:ROWS, :] = jnp.zeros((ROWS - 128, LANES), F32)
        narrow[b, 128:PACKED, 0:LANES] = jnp.zeros((PACKED - 128, LANES), BF16)
    loads[0].wait()
    for b in range(CX):
        for row in range(0, 128, 16):
            value = state[pl.ds(row * CX + b, 16, stride=CX), :]
            wide[b + 2, row : row + 16, :] = value
            narrow[b, row : row + 16, 0:LANES] = value.astype(BF16)
        value = state[pl.ds(128 * CX + b, COMPS - 128, stride=CX), :]
        wide[b + 2, 128:COMPS, :] = value
        narrow[b, 128:ROWS, 0:LANES] = wide[b + 2, 128:ROWS, :].astype(BF16)
    lane = iota((48, LANES), 1)
    for row in range(0, PACKED, 48):
        total = edges(lambda b: narrow[b, row : row + 48, 0:LANES], 48, BF16)
        for side in range(2):
            ys[0, side, row : row + 48, :] = one_side(side, lane, total)
    for side in range(2):
        ys[1, side, 128:PACKED, :] = jnp.zeros((PACKED - 128, LANES), BF16)
    pack_x(0)
    pl.semaphore_wait(barrier, 4)
    for side in (2, 3, 0, 1):
        copy(0, side).start()

    cells[...] = jnp.zeros_like(cells)
    cells16[...] = jnp.zeros_like(cells16)
    edge_cells[...] = jnp.zeros_like(edge_cells)
    edge_cells16[...] = jnp.zeros_like(edge_cells16)
    gained[0:40, :] = jnp.zeros((40, HALF), F32)
    edge_gained[0:40, :] = jnp.zeros((40, LANES), F32)
    edge_gained[ROWS - 8 :, :] = jnp.zeros((8, LANES), F32)
    gained[ROWS - 8 :, :] = jnp.zeros((8, HALF), F32)
    for load in loads[1:]:
        load.wait()
    for b in range(CX):
        found = jnp.int32(0)
        for k in range(CX):
            hit = (order[0, 0, k] == b) & (k < count[0, 0])
            found = found + hit.astype(jnp.int32)
        cloudy[b] = found.astype(F32)
    lane = iota((8, LANES), 1)
    shares = jnp.zeros((8, LANES), F32)
    for b in range(CX):
        for at in (8 * b, 64 + 8 * b):
            shares = shares + jnp.where((lane >= at) & (lane < at + 8), 1.0, 0.0) * cloudy[b]
    share[...] = shares
    build_weights(cx, cy, weights)
    build_bands(weights, bands)
    stack_gain(gain, stacked)
    exchange(stacked, chooser)
    build_gain(stacked, matrix, corner, corner.at[PACKED : PACKED + 48, 0:LANES])
    build_loss(loss, square, table)
    corner16[...] = corner[...].astype(BF16)
    table16[...] = table[...].astype(BF16)

    for step in range(2):
        for side in range(4):
            copy(step, side).wait_recv()
        for column in range(2):
            wide[column] = xr[step, 1, column, 0:ROWS, :].astype(F32)
            wide[CX + 2 + column] = xr[step, 0, column, 0:ROWS, :].astype(F32)
        halo = yr[step, 0] + yr[step, 1]
        for b in range(CX):
            narrow[b, :, LANES : 2 * LANES] = halo
        transport(wide, narrow, bands, weights, moved, cells, cells16)

        if step == 0:
            gather_edges(moved, edge, edge_cells, edge_cells16)

            def finish_edge(pos, row, change):
                n = change.shape[0]
                value = edge[row : row + n, :] + change * share[0:1, :]
                value, lane = value.astype(BF16), iota((n, LANES), 1)
                for side in range(2):
                    ys[1, side, row : row + n, :] = one_side(side, lane, value)

            collide(
                0, matrix, corner16, table16, edge_cells, edge_cells16, edge_gained, finish_edge
            )
            for side in range(2, 4):
                copy(1, side).start()

        def collide_half(half):
            def finish(pos, row, change):
                b = (4 * half + pos + 6) % 8
                n = change.shape[0]
                value = moved[b, row : row + n, :] + change * cloudy[b]
                if step == 0:
                    wide[b + 2, row : row + n, :] = value
                    narrow[b, row : row + n, 0:LANES] = value.astype(BF16)
                else:
                    n = min(n, COMPS - row)
                    out[pl.ds(row * CX + b, n, stride=CX), :] = value[0:n]

            collide(half, matrix, corner16, table16, cells, cells16, gained, finish)

        if step == 0:
            collide_half(0)
            pack_x(1)
            for side in range(2):
                copy(1, side).start()
            collide_half(1)
        else:
            collide_half(0)
            collide_half(1)
    for step in range(2):
        for side in range(4):
            copy(step, side).wait_send()


def pinned(array):
    return pltpu.with_memory_space_constraint(array, pltpu.HBM)


def per_device(bin_state, courant_x, courant_y, cloudy_order, block_count, gain_kernel, loss_rate):
    vmem = pl.BlockSpec(memory_space=pltpu.VMEM)
    hbm = pl.BlockSpec(memory_space=pltpu.HBM)
    flat = bin_state.reshape(COMPS * CX, LANES)
    result = pl.pallas_call(
        kernel,
        out_shape=jax.ShapeDtypeStruct(flat.shape, F32),
        in_specs=[hbm] * 4 + [pl.BlockSpec(memory_space=pltpu.VMEM)] + [hbm] * 2,
        out_specs=vmem,
        scratch_shapes=[
            pltpu.VMEM(flat.shape, F32),
            pltpu.VMEM(courant_x.shape, F32),
            pltpu.VMEM(courant_y.shape, F32),
            pltpu.SMEM(cloudy_order.shape, jnp.int32),
            pltpu.VMEM(gain_kernel.shape, BF16),
            pltpu.VMEM(loss_rate.shape, BF16),
            pltpu.VMEM((CX + 4, ROWS, LANES), F32),
            pltpu.VMEM((CX, PACKED, 2 * LANES), BF16),
            pltpu.VMEM((CX, ROWS, LANES), F32),
            pltpu.VMEM((2, 152, HALF), F32),
            pltpu.VMEM((2, 256, HALF), BF16),
            pltpu.VMEM((480, WIDE), BF16),
            pltpu.VMEM((WIDE, 384), BF16),
            pltpu.VMEM((len(GROUPS) * SLAB, 256), BF16),
            pltpu.VMEM((PACKED + 48, 256), F32),
            pltpu.VMEM((PACKED + 48, 256), BF16),
            pltpu.VMEM((LANES, LANES), F32),
            pltpu.VMEM((PACKED, 256), F32),
            pltpu.VMEM((PACKED, 256), BF16),
            pltpu.VMEM((ROWS, HALF), F32),
            pltpu.VMEM((9, CX, LANES), F32),
            pltpu.VMEM((CX, 2 * LANES, LANES), BF16),
            pltpu.SMEM((CX,), F32),
            pltpu.VMEM((8, LANES), F32),
            pltpu.VMEM((ROWS, LANES), F32),
            pltpu.VMEM((1, 152, LANES), F32),
            pltpu.VMEM((1, 2 * LANES, LANES), BF16),
            pltpu.VMEM((ROWS, LANES), F32),
            pltpu.VMEM((2, 2, 2, PACKED, LANES), BF16),
            pltpu.VMEM((2, 2, PACKED, LANES), BF16),
            pltpu.VMEM((2, 2, 2, PACKED, LANES), BF16),
            pltpu.VMEM((2, 2, PACKED, LANES), BF16),
            pltpu.SemaphoreType.DMA((6,)),
            pltpu.SemaphoreType.DMA((2, 4)),
            pltpu.SemaphoreType.DMA((2, 4)),
        ],
        compiler_params=pltpu.CompilerParams(
            collective_id=0, has_side_effects=True, vmem_limit_bytes=24 * 1024 * 1024
        ),
        name="microphysics",
    )(
        pinned(flat), pinned(courant_x), pinned(courant_y), pinned(cloudy_order), block_count,
        pinned(gain_kernel), pinned(loss_rate),
    )
    return result.reshape(bin_state.shape)


def solution(mesh):
    placed = (
        P(None, "gx", "gy"),
        P("gx", "gy"),
        P("gx", "gy"),
        P("gx", "gy", None),
        P("gy", "gx"),
        P(),
        P(),
    )
    return jax.shard_map(
        per_device, mesh=mesh, in_specs=placed, out_specs=P(None, "gx", "gy"), check_vma=False
    )
```

```python
import jax
import jax.numpy as jnp
import numpy as np
from jax import lax
from jax.experimental import pallas as pl
from jax.experimental.pallas import tpu as pltpu
from jax.sharding import PartitionSpec as P

BINS = 33
COMPS = 132
ROWS = 136
PACKED = 144
LEV = 4
CX = 8
LANES = 128
HALF = 512
FLAT = BINS * BINS
WIDE = 1152
MESH = pl.DeviceIdType.MESH
F32, BF16 = jnp.float32, jnp.bfloat16

OFFSET = (0, 33, 66, 128)
STACK = (3, 6, 8, 5, 0, 1, 2, 4, 7, 9)
SWAPPED = 4
PLACE = {p: s for s, p in enumerate(STACK)}
GROUPS = (
    (1, 0, ((0, 0), (1, 1))),
    (1, 1, ((4, 1),)),
    (2, 0, ((2, 2),)),
    (3, 2, ((5, 1), (7, 2))),
    (3, 3, ((3, 0), (6, 1), (8, 2), (9, 3))),
)
PAIR_OF = {(0, 0): 0, (0, 1): 1, (0, 2): 2, (0, 3): 3, (1, 1): 4, (1, 2): 5, (1, 3): 6, (2, 2): 7, (2, 3): 8, (3, 3): 9}
CHUNK = 11
SLAB = BINS * 32
PARTS = ((0, 48), (48, 48), (96, 40))


def iota(shape, dim):
    return lax.broadcasted_iota(jnp.int32, shape, dim)


def stack_gain(gain, stacked):
    stacked[...] = jnp.zeros_like(stacked)
    for place, pair in enumerate(STACK):
        stacked[place * 48 : place * 48 + BINS, 0:FLAT] = gain[pair]


def exchange(stacked, chooser):
    rows = SWAPPED * 48
    source = stacked[0:rows, :]
    width = 384
    parts = []
    for part in range(WIDE // width):
        column = iota((1, width), 1) + part * width
        high = (column * 1986) >> 16
        origin = jnp.where(column < FLAT, (column - high * BINS) * BINS + high, -1)
        chooser[...] = jnp.where(iota((WIDE, width), 0) == origin, 1.0, 0.0).astype(BF16)
        parts.append(
            jnp.dot(source, chooser[...], preferred_element_type=F32).astype(BF16)
        )
    for part in range(WIDE // width):
        stacked[0:rows, part * width : (part + 1) * width] = parts[part]


def window(stacked, lane, pair, index, lane0):
    row = PLACE[pair] * 48
    start = index * BINS
    tile, off = start // LANES, start % LANES
    shift = (lane0 - off) % LANES
    def moved(t):
        value = stacked[row : row + 48, t * LANES : (t + 1) * LANES]
        return pltpu.roll(value, shift, 1) if shift else value
    first = moved(tile)
    if off + BINS <= LANES:
        return first
    return jnp.where(lane < lane0 + LANES - off, first, moved(tile + 1))


def build_gain(stacked, matrix, corner, corner2):
    lane = iota((48, LANES), 1)
    inside = {at % LANES: (lane >= at % LANES) & (lane < at % LANES + BINS) for at in OFFSET}
    nothing = jnp.zeros((48, LANES), BF16)
    corner[...] = jnp.zeros_like(corner)
    corner2[...] = jnp.zeros_like(corner2)
    for group, (target, factor, pairs) in enumerate(GROUPS):
        for index in range(BINS):
            low, high = None, None
            for pair, cls in sorted(pairs, key=lambda entry: entry[1]):
                lane0 = OFFSET[cls] % LANES
                piece = window(stacked, lane, pair, index, lane0)
                if cls == 3:
                    high = jnp.where(inside[lane0], piece, nothing)
                else:
                    low = jnp.where(inside[lane0], piece, nothing if low is None else low)
            row = group * SLAB + index * 32
            for value, col in ((low, 0), (high, LANES)):
                if value is None:
                    continue
                matrix[row : row + 32, col : col + LANES] = value[0:32]
                last = value[32:48].astype(F32)[0:1]
                if target == 2:
                    corner2[index : index + 1, :] = last
                else:
                    at = factor * BINS + index
                    corner[at : at + 1, col : col + LANES] = last


def build_loss(loss, square, table):
    table[...] = jnp.zeros_like(table)
    square[...] = jnp.zeros_like(square)
    for (a, b), pair in PAIR_OF.items():
        square[0:BINS, 0:BINS] = loss[pair].astype(F32)
        plain = square[...]
        turned = plain.T
        if a == b:
            plain = plain + turned
        table[a * BINS : a * BINS + BINS, OFFSET[b] : OFFSET[b] + BINS] = plain[0:BINS, 0:BINS]
        if a != b:
            table[b * BINS : b * BINS + BINS, OFFSET[a] : OFFSET[a] + BINS] = turned[0:BINS, 0:BINS]


def build_weights(cx, cy, weights):
    own = jnp.ones((CX, LANES), F32)
    for axis, ref in enumerate((cx, cy)):
        c = ref[...]
        up = c > 0.0
        weights[axis * 4 + 0] = c * jnp.where(up, 1.0 / 3.0, 1.0)
        weights[axis * 4 + 1] = c * jnp.where(up, 0.0, -1.0 / 6.0)
        weights[axis * 4 + 2] = c * jnp.where(up, -1.0, -1.0 / 3.0)
        weights[axis * 4 + 3] = c * jnp.where(up, 1.0 / 6.0, 0.0)
        own = own - c * jnp.where(up, 0.5, -0.5)
    weights[8] = own


def build_bands(weights, bands):
    def block(b, carry):
        row, lane = iota((LANES, LANES), 0), iota((LANES, LANES), 1)
        left, right = row - 8 * b, row - 64 - 8 * b
        far = jnp.full_like(row, -1000)
        outer = jnp.where((left >= 0) & (left < 8), left - 8, far)
        outer = jnp.where((right >= 0) & (right < 8), right + LANES, outer)
        for part, place in ((0, row), (1, outer)):
            value = jnp.zeros((LANES, LANES), F32)
            for k, shift in ((4, LEV), (5, 2 * LEV), (6, -LEV), (7, -2 * LEV)):
                value = jnp.where(place - lane == shift, -weights[k, pl.ds(b, 1), :], value)
            bands[b, part * LANES : (part + 1) * LANES, :] = value.astype(BF16)
        return carry

    lax.fori_loop(0, CX, block, 0)


def edges(block, n, dtype):
    lane = iota((n, LANES), 1)
    total = jnp.zeros((n, LANES), dtype)
    for b in range(CX):
        value = block(b)
        for at, shift in ((8 * b, 8 * b + 8), (64 + 8 * b, 64 + 8 * b)):
            total = jnp.where((lane >= at) & (lane < at + 8), pltpu.roll(value, shift, 1), total)
    return total


def one_side(side, lane, total):
    return jnp.where(lane >= 64 if side == 0 else lane < 64, total, jnp.zeros_like(total))


def place(total, row, n, half, cells, cells16, cols):
    rows = slice(row, row + n)
    rounded = total.astype(BF16)
    cells[half, rows, cols] = rounded.astype(F32)
    if row < 96:
        cells16[half, rows, cols] = rounded
    else:
        kept = jnp.where(iota((16, LANES), 0) < 3, total[0:16], 0.0)
        cells16[half, 96:112, cols] = kept.astype(BF16)
        cells16[half, 128:176, cols] = cells[half, 99:147, cols].astype(BF16)


def transport(places, wide, narrow, bands, weights, moved, cells, cells16):
    for pos in places:
        b = (pos + 6) % 8
        half, cols = pos // 4, slice((pos % 4) * LANES, (pos % 4 + 1) * LANES)
        w = [weights[k, b : b + 1, :] for k in (0, 1, 2, 3, 8)]
        flux = jnp.dot(narrow[b], bands[b], preferred_element_type=F32)
        for row, n in PARTS:
            rows = slice(row, row + n)
            total = w[4] * wide[b + 2, rows, :] + flux[rows]
            total = total - w[0] * wide[b + 3, rows, :] - w[1] * wide[b + 4, rows, :]
            total = total - w[2] * wide[b + 1, rows, :] - w[3] * wide[b, rows, :]
            total = jnp.maximum(total, 0.0)
            moved[b, rows, :] = total
            place(total, row, n, half, cells, cells16, cols)


def gather_edges(moved, edge, cells, cells16):
    for row, n in PARTS:
        total = edges(lambda b: moved[b, row : row + n, :], n, F32)
        edge[row : row + n, :] = total
        place(total, row, n, 0, cells, cells16, slice(0, LANES))


def collide(half, matrix, corner16, table16, cells, cells16, gained, finish):
    total, width = {}, cells.shape[2]
    for group, (target, factor, pairs) in enumerate(GROUPS):
        depth = 256 if any(cls == 3 for _, cls in pairs) else 128
        for first in range(0, BINS, CHUNK):
            row = group * SLAB + first * 32
            part = jnp.dot(
                matrix[row : row + CHUNK * 32, 0:depth],
                cells16[half, 0:depth, :],
                preferred_element_type=F32,
            )
            for k in range(CHUNK):
                at = factor * BINS + first + k
                term = cells[half, at : at + 1, :] * part[32 * k : 32 * k + 32]
                total[target] = total[target] + term if target in total else term
    for target in (1, 2, 3):
        gained[target * BINS : target * BINS + 32, :] = total[target]
    last = jnp.dot(corner16[...], cells16[half], preferred_element_type=F32)
    ends = last[0:ROWS] * cells[half, 0:ROWS, :]
    below = iota((ROWS, width), 0) < 2 * BINS
    gained[65:66, :] = jnp.sum(jnp.where(below, ends, 0.0), axis=0, keepdims=True)
    gained[131:132, :] = jnp.sum(jnp.where(below, 0.0, ends), axis=0, keepdims=True)
    second = last[PACKED : PACKED + 40] * cells[half, 0:40, :]
    gained[98:99, :] = jnp.sum(second, axis=0, keepdims=True)
    lost = jnp.dot(table16[...], cells16[half], preferred_element_type=F32)
    for pos in range(width // LANES):
        col = slice(pos * LANES, (pos + 1) * LANES)
        for row, n in PARTS:
            rows = slice(row, row + n)
            change = gained[rows, col] - cells[half, rows, col] * lost[rows, col]
            finish(pos, row, change.astype(BF16).astype(F32))


def kernel(
    state_hbm, cx_hbm, cy_hbm, order_hbm, count, gain_hbm, loss_hbm, out,
    state, cx, cy, order, gain, loss,
    wide, narrow, moved, cells, cells16, stacked, chooser, matrix, corner, corner16, square, table, table16,
    gained, weights, bands, cloudy, share, edge, edge_cells, edge_cells16, edge_gained, xs, ys, xr, yr, load_sem, send_sem, recv_sem,
):
    gx, gy = lax.axis_index("gx"), lax.axis_index("gy")
    nx, ny = lax.axis_size("gx"), lax.axis_size("gy")
    peers = (
        (lax.rem(gx + nx - 1, nx), gy),
        (lax.rem(gx + 1, nx), gy),
        (gx, lax.rem(gy + ny - 1, ny)),
        (gx, lax.rem(gy + 1, ny)),
    )
    loads = [
        pltpu.make_async_copy(source, kept, load_sem.at[k])
        for k, (source, kept) in enumerate(
            (
                (state_hbm, state), (cx_hbm, cx), (cy_hbm, cy), (order_hbm, order),
                (gain_hbm, gain), (loss_hbm, loss),
            )
        )
    ]
    for load in loads:
        load.start()
    barrier = pltpu.get_barrier_semaphore()
    for peer in peers:
        pl.semaphore_signal(barrier, inc=1, device_id=peer, device_id_type=MESH)

    def copy(step, side):
        sent, kept = (xs, xr) if side < 2 else (ys, yr)
        return pltpu.make_async_remote_copy(
            src_ref=sent.at[step, side % 2],
            dst_ref=kept.at[step, side % 2],
            send_sem=send_sem.at[step, side],
            recv_sem=recv_sem.at[step, side],
            device_id=peers[side],
            device_id_type=MESH,
        )

    def pack_x(step):
        for side in range(2):
            for column in range(2):
                xs[step, side, column] = narrow[6 * side + column, :, 0:LANES]

    for b in range(CX):
        wide[b + 2, 128:ROWS, :] = jnp.zeros((ROWS - 128, LANES), F32)
        narrow[b, 128:PACKED, 0:LANES] = jnp.zeros((PACKED - 128, LANES), BF16)
    loads[0].wait()
    for b in range(CX):
        for row in range(0, 128, 16):
            value = state[pl.ds(row * CX + b, 16, stride=CX), :]
            wide[b + 2, row : row + 16, :] = value
            narrow[b, row : row + 16, 0:LANES] = value.astype(BF16)
        value = state[pl.ds(128 * CX + b, COMPS - 128, stride=CX), :]
        wide[b + 2, 128:COMPS, :] = value
        narrow[b, 128:ROWS, 0:LANES] = wide[b + 2, 128:ROWS, :].astype(BF16)
    lane = iota((48, LANES), 1)
    for row in range(0, PACKED, 48):
        total = edges(lambda b: narrow[b, row : row + 48, 0:LANES], 48, BF16)
        for side in range(2):
            ys[0, side, row : row + 48, :] = one_side(side, lane, total)
    for side in range(2):
        ys[1, side, 128:PACKED, :] = jnp.zeros((PACKED - 128, LANES), BF16)
    pack_x(0)
    pl.semaphore_wait(barrier, 4)
    for side in (2, 3, 0, 1):
        copy(0, side).start()

    cells[...] = jnp.zeros_like(cells)
    cells16[...] = jnp.zeros_like(cells16)
    edge_cells[...] = jnp.zeros_like(edge_cells)
    edge_cells16[...] = jnp.zeros_like(edge_cells16)
    gained[0:40, :] = jnp.zeros((40, HALF), F32)
    edge_gained[0:40, :] = jnp.zeros((40, LANES), F32)
    edge_gained[ROWS - 8 :, :] = jnp.zeros((8, LANES), F32)
    gained[ROWS - 8 :, :] = jnp.zeros((8, HALF), F32)
    for load in loads[1:]:
        load.wait()
    for b in range(CX):
        found = jnp.int32(0)
        for k in range(CX):
            hit = (order[0, 0, k] == b) & (k < count[0, 0])
            found = found + hit.astype(jnp.int32)
        cloudy[b] = found.astype(F32)
    lane = iota((8, LANES), 1)
    shares = jnp.zeros((8, LANES), F32)
    for b in range(CX):
        for at in (8 * b, 64 + 8 * b):
            shares = shares + jnp.where((lane >= at) & (lane < at + 8), 1.0, 0.0) * cloudy[b]
    share[...] = shares
    build_weights(cx, cy, weights)
    build_bands(weights, bands)
    stack_gain(gain, stacked)
    exchange(stacked, chooser)
    build_gain(stacked, matrix, corner, corner.at[PACKED : PACKED + 48, 0:LANES])
    build_loss(loss, square, table)
    corner16[...] = corner[...].astype(BF16)
    table16[...] = table[...].astype(BF16)

    for step in range(2):

        def columns_arrive():
            for side in range(2):
                copy(step, side).wait_recv()
            for column in range(2):
                wide[column] = xr[step, 1, column, 0:ROWS, :].astype(F32)
                wide[CX + 2 + column] = xr[step, 0, column, 0:ROWS, :].astype(F32)

        def move(places):
            transport(places, wide, narrow, bands, weights, moved, cells, cells16)

        if step == 0:
            columns_arrive()
        for side in range(2, 4):
            copy(step, side).wait_recv()
        halo = yr[step, 0] + yr[step, 1]
        for b in range(CX):
            narrow[b, :, LANES : 2 * LANES] = halo
        if step == 0:
            move(range(CX))
        if step == 0:
            gather_edges(moved, edge, edge_cells, edge_cells16)

            def finish_edge(pos, row, change):
                n = change.shape[0]
                value = edge[row : row + n, :] + change * share[0:1, :]
                value, lane = value.astype(BF16), iota((n, LANES), 1)
                for side in range(2):
                    ys[1, side, row : row + n, :] = one_side(side, lane, value)

            collide(
                0, matrix, corner16, table16, edge_cells, edge_cells16, edge_gained, finish_edge
            )
            for side in range(2, 4):
                copy(1, side).start()

        def collide_half(half):
            def finish(pos, row, change):
                b = (4 * half + pos + 6) % 8
                n = change.shape[0]
                value = moved[b, row : row + n, :] + change * cloudy[b]
                if step == 0:
                    wide[b + 2, row : row + n, :] = value
                    narrow[b, row : row + n, 0:LANES] = value.astype(BF16)
                else:
                    n = min(n, COMPS - row)
                    out[pl.ds(row * CX + b, n, stride=CX), :] = value[0:n]

            collide(half, matrix, corner16, table16, cells, cells16, gained, finish)

        if step == 0:
            collide_half(0)
            pack_x(1)
            for side in range(2):
                copy(1, side).start()
            collide_half(1)
        else:
            move(range(4, CX))
            collide_half(1)
            columns_arrive()
            move(range(4))
            collide_half(0)
    for step in range(2):
        for side in range(4):
            copy(step, side).wait_send()


def pinned(array):
    return pltpu.with_memory_space_constraint(array, pltpu.HBM)


def per_device(bin_state, courant_x, courant_y, cloudy_order, block_count, gain_kernel, loss_rate):
    vmem = pl.BlockSpec(memory_space=pltpu.VMEM)
    hbm = pl.BlockSpec(memory_space=pltpu.HBM)
    flat = bin_state.reshape(COMPS * CX, LANES)
    result = pl.pallas_call(
        kernel,
        out_shape=jax.ShapeDtypeStruct(flat.shape, F32),
        in_specs=[hbm] * 4 + [pl.BlockSpec(memory_space=pltpu.VMEM)] + [hbm] * 2,
        out_specs=vmem,
        scratch_shapes=[
            pltpu.VMEM(flat.shape, F32),
            pltpu.VMEM(courant_x.shape, F32),
            pltpu.VMEM(courant_y.shape, F32),
            pltpu.SMEM(cloudy_order.shape, jnp.int32),
            pltpu.VMEM(gain_kernel.shape, BF16),
            pltpu.VMEM(loss_rate.shape, BF16),
            pltpu.VMEM((CX + 4, ROWS, LANES), F32),
            pltpu.VMEM((CX, PACKED, 2 * LANES), BF16),
            pltpu.VMEM((CX, ROWS, LANES), F32),
            pltpu.VMEM((2, 152, HALF), F32),
            pltpu.VMEM((2, 256, HALF), BF16),
            pltpu.VMEM((480, WIDE), BF16),
            pltpu.VMEM((WIDE, 384), BF16),
            pltpu.VMEM((len(GROUPS) * SLAB, 256), BF16),
            pltpu.VMEM((PACKED + 48, 256), F32),
            pltpu.VMEM((PACKED + 48, 256), BF16),
            pltpu.VMEM((LANES, LANES), F32),
            pltpu.VMEM((PACKED, 256), F32),
            pltpu.VMEM((PACKED, 256), BF16),
            pltpu.VMEM((ROWS, HALF), F32),
            pltpu.VMEM((9, CX, LANES), F32),
            pltpu.VMEM((CX, 2 * LANES, LANES), BF16),
            pltpu.SMEM((CX,), F32),
            pltpu.VMEM((8, LANES), F32),
            pltpu.VMEM((ROWS, LANES), F32),
            pltpu.VMEM((1, 152, LANES), F32),
            pltpu.VMEM((1, 2 * LANES, LANES), BF16),
            pltpu.VMEM((ROWS, LANES), F32),
            pltpu.VMEM((2, 2, 2, PACKED, LANES), BF16),
            pltpu.VMEM((2, 2, PACKED, LANES), BF16),
            pltpu.VMEM((2, 2, 2, PACKED, LANES), BF16),
            pltpu.VMEM((2, 2, PACKED, LANES), BF16),
            pltpu.SemaphoreType.DMA((6,)),
            pltpu.SemaphoreType.DMA((2, 4)),
            pltpu.SemaphoreType.DMA((2, 4)),
        ],
        compiler_params=pltpu.CompilerParams(
            collective_id=0, has_side_effects=True, vmem_limit_bytes=24 * 1024 * 1024
        ),
        name="microphysics",
    )(
        pinned(flat), pinned(courant_x), pinned(courant_y), pinned(cloudy_order), block_count,
        pinned(gain_kernel), pinned(loss_rate),
    )
    return result.reshape(bin_state.shape)


def solution(mesh):
    placed = (
        P(None, "gx", "gy"),
        P("gx", "gy"),
        P("gx", "gy"),
        P("gx", "gy", None),
        P("gy", "gx"),
        P(),
        P(),
    )
    return jax.shard_map(
        per_device, mesh=mesh, in_specs=placed, out_specs=P(None, "gx", "gy"), check_vma=False
    )
```
